32 devices in a mesh: vox: 16 (over z, x, core), subj: 2 (over y).
Axes of the slice: x: 2, y: 2, z: 4, core: 2. Of those that a mesh axis runs over, the one named last changes fastest.
Arguments:
- series: bfloat16 [8, 4096, 512], P('subj', 'vox'), may hold values from -6 to 6
- live_mask: int32 [4096], P('vox'), may hold values from 0 to 1, as said below
- neighbours: int32 [4096, 13], P('vox'), may hold values from -1 to 510, as said below
- start_vectors: float32 [4096, 64], P('vox'), may hold values from -60 to 60
Outputs:
- embedding: float32 [4096, 64], P('vox')
The draws below stay inside these ranges and needn't reach their ends.
Inputs may be any that keep to these rules, and one draw needn't show every extreme that they name: `live_mask`: within each aligned block of 128 voxel slots the live slots are a leading run of 1 to 128 slots. `neighbours`: slot n of voxel i names voxel (i // 256 - 1) * 256 + n, which is live and lies before i; the entries of a row are distinct or -1; rows of dead voxels are all -1; rows of the first 256 voxels name no slot under 256.
All inputs are finite; a program needn't handle non-finite values.
Results may differ from the reference program's by a relative error of at most 0.0024.
Values may be sent and summed in bfloat16 or wider, within the bound.
No kernel may reach another device: no remote copies, remote signals or barrier semaphores. Data moves between devices by JAX's collectives and lax.ppermute only.
A program may use at most 64 MiB of HBM per device.

```python
import math
import jax
import jax.numpy as jnp
from jax import lax

VOX_DEV = 256
FRAMES = 512
VECS = 64
OFFSETS = 13
BLOCK = 128
ITERS = 3
VOXELS = 4096
SUBJECTS = 8


def brain_layout(key):
    first, second = jax.random.split(jax.random.fold_in(key, 7))
    blocks = VOXELS // BLOCK
    filled = jax.random.randint(first, (blocks,), 1, BLOCK + 1)
    within = jnp.arange(BLOCK, dtype=jnp.int32)
    living = (within[None, :] < filled[:, None]).reshape(-1).astype(jnp.int32)
    position = jnp.arange(VOXELS, dtype=jnp.int32)
    stride = VOX_DEV // OFFSETS
    lowest = jnp.arange(OFFSETS, dtype=jnp.int32) * stride + 1
    distance = lowest[None, :] + jax.random.randint(second, (VOXELS, OFFSETS), 0, stride)
    target = position[:, None] - distance
    usable = (target >= 0) & (living[jnp.maximum(target, 0)] == 1) & (living[:, None] == 1)
    local_slot = VOX_DEV + (position % VOX_DEV)[:, None] - distance
    return (living, jnp.where(usable, local_slot, -1).astype(jnp.int32))


def draw_live_mask(key, part):
    return brain_layout(key)[0]


def draw_neighbours(key, part):
    return brain_layout(key)[1]


def draw_start_vectors(key, part):
    first = jax.random.fold_in(jax.random.fold_in(key, 11), 0)
    fraction = jnp.arange(VOXELS, dtype=jnp.float32) / VOXELS
    noise = jnp.clip(jax.random.normal(first, (VOXELS, VECS), jnp.float32), -6.0, 6.0)
    rows = (1.0 + 3.0 * fraction)[:, None]
    return noise * rows


def block_levels(stream_key, shape, pieces, low, largest):
    def one(dim, blocks):
        draws = jax.random.uniform(jax.random.fold_in(jax.random.fold_in(stream_key, 6), dim), (blocks,), jnp.float32, low / len(pieces), largest / len(pieces))
        return jnp.repeat(jnp.exp(draws), shape[dim] // blocks).reshape((-1,) + (1,) * (len(shape) - dim - 1))

    level = one(*pieces[0])
    for cut in pieces[1:]:
        level = level * one(*cut)
    return level


def scatter_about(stream_key, shape, scale, bound, cuts=(), kind=jnp.bfloat16):
    result = scale * jax.random.normal(stream_key, shape, jnp.float32)
    if cuts:
        result = result * block_levels(stream_key, shape, cuts, -0.22, 0.18)
    return jnp.clip(result, -bound, bound).astype(kind)


def setup_inputs(seed: int = 0) -> dict:
    splits = jax.random.split(jax.random.key(seed), 5)
    return {
        "series": scatter_about(splits[0], (SUBJECTS, VOXELS, FRAMES), 1.0, 6.0, ((0, 2), (1, 16))),
        "live_mask": draw_live_mask(jax.random.fold_in(splits[4], 71), 0),
        "neighbours": draw_neighbours(jax.random.fold_in(splits[4], 71), 0),
        "start_vectors": draw_start_vectors(jax.random.fold_in(splits[4], 71), 0),
    }


def standard(block):
    values = block.astype(jnp.float32)
    center = values - lax.optimization_barrier(jnp.mean(values, axis=-1, keepdims=True))
    spread = lax.optimization_barrier(jnp.mean(center * center, axis=-1, keepdims=True))
    return (center * lax.rsqrt(spread + 1e-05)).astype(jnp.bfloat16)

def reference(series, live_mask, neighbours, start_vectors):
    position = jnp.arange(VOXELS, dtype=jnp.int32)
    present = neighbours >= 0
    global_index = jnp.where(present, ((position // VOX_DEV - 1) * VOX_DEV)[:, None] + neighbours, 0).astype(jnp.int32)

    def one_subject(summed, block):
        zscored = standard(block).astype(jnp.float32)
        columns = []
        for offset in range(OFFSETS):
            columns.append(lax.optimization_barrier(jnp.sum(zscored * zscored[global_index[:, offset]], axis=1)))
        return (summed + jnp.stack(columns, axis=1), None)
    summed, _ = lax.scan(one_subject, jnp.zeros((VOXELS, OFFSETS), jnp.float32), series)
    weight = jnp.where(present, jnp.exp(0.5 * summed / math.sqrt(FRAMES * SUBJECTS)), 0.0)
    flat_index = global_index.reshape(-1)
    degree = 1.0 + lax.optimization_barrier(jnp.sum(weight, axis=1)) + jax.ops.segment_sum(weight.reshape(-1), flat_index, num_segments=VOXELS)
    living = live_mask.astype(jnp.float32)
    scaling = living * lax.rsqrt(degree)
    vectors = living[:, None] * start_vectors
    for repeat in range(ITERS):
        scaled = scaling[:, None] * vectors
        forward = lax.optimization_barrier(jnp.sum(weight[:, :, None] * scaled[global_index], axis=1))
        returns = jax.ops.segment_sum((weight[:, :, None] * scaled[:, None, :]).reshape(-1, VECS), flat_index, num_segments=VOXELS)
        images = 0.5 * (vectors + scaling[:, None] * (scaled + forward + returns))
        gram_matrix = jnp.dot(images.T, images, precision=lax.Precision.HIGHEST)
        factor = jnp.linalg.cholesky(gram_matrix)
        vectors = lax.linalg.triangular_solve(factor, images, left_side=False, lower=True, transpose_a=True)
    return vectors
```

```python
import math

import jax
import jax.numpy as jnp
from jax import lax
from jax.sharding import PartitionSpec as P

ITERS = 3


def shifted(shard, axis, by):
    count = lax.axis_size(axis)
    pairs = [(i, i + by) for i in range(count) if 0 <= i + by < count]
    return lax.ppermute(shard, axis, pairs)


def exchanged(value, axis, distance):
    count = lax.axis_size(axis)
    return lax.ppermute(value, axis, [(i, i ^ distance) for i in range(count)])


def summed_over(value, axis):
    count = lax.axis_size(axis)
    if count & (count - 1):
        return lax.psum(value, axis)
    stride = 1
    while stride < count:
        if stride > 1 and 4 * stride <= count:
            first, second, third = (exchanged(value, axis, k * stride) for k in (1, 2, 3))
            value = (value + first) + (second + third)
            stride *= 4
        else:
            value = value + exchanged(value, axis, stride)
            stride *= 2
    return value


def as_sent(shard):
    return jax.tree.map(lambda a: a.astype(jnp.bfloat16) if a.dtype == jnp.float32 else a, shard)


def standard(block):
    values = block.astype(jnp.float32)
    center = values - jnp.mean(values, axis=-1, keepdims=True)
    spread = jnp.mean(center * center, axis=-1, keepdims=True)
    return (center * lax.rsqrt(spread + 1e-05)).astype(jnp.bfloat16)


def orthonormal(images):
    gram_matrix = jnp.dot(images.T, images, precision=lax.Precision.HIGHEST)
    gram_matrix = summed_over(gram_matrix, "vox")
    factor = jnp.linalg.cholesky(gram_matrix)
    return lax.linalg.triangular_solve(
        factor, images, left_side=False, lower=True, transpose_a=True
    )


def dense_graph(weight, slots, columns_total):
    column_ids = jnp.arange(columns_total, dtype=jnp.int32)
    matrix = jnp.zeros((weight.shape[0], columns_total), jnp.float32)
    for offset in range(weight.shape[1]):
        hits = (slots[:, offset][:, None] == column_ids[None, :]).astype(jnp.float32)
        matrix = matrix + weight[:, offset][:, None] * hits
    return matrix


def product(left, right):
    return jnp.dot(left, right, precision=lax.Precision.HIGHEST)


def on_device(series, live_mask, neighbours, start_vectors):
    voxels_here = series.shape[1]
    frames = series.shape[2]
    subjects = series.shape[0] * lax.axis_size("subj")
    scale_factor = 0.5 / math.sqrt(frames * subjects)
    zscored = standard(series)
    earlier = shifted(zscored, "vox", 1)
    window = jnp.concatenate([earlier, zscored], axis=1)
    present = neighbours >= 0
    safe_slots = jnp.maximum(neighbours, 0)
    columns = []
    for offset in range(neighbours.shape[1]):
        picked = jnp.take(window, safe_slots[:, offset], axis=1)
        columns.append(
            jnp.einsum("svf,svf->v", zscored, picked, preferred_element_type=jnp.float32)
        )
    partial_sums = jnp.stack(columns, axis=1)
    summed = lax.psum(partial_sums, "subj")
    weight = jnp.where(present, jnp.exp(scale_factor * summed), 0.0)
    living = live_mask.astype(jnp.float32)
    local_graph = dense_graph(weight, neighbours, 2 * voxels_here)
    owed = jnp.sum(local_graph, axis=0)
    received = shifted(owed[:voxels_here], "vox", -1)
    degree = 1.0 + jnp.sum(weight, axis=1) + owed[voxels_here:] + received
    scaling = living * lax.rsqrt(degree)
    vectors = living[:, None] * start_vectors
    for repeat in range(ITERS):
        scaled = scaling[:, None] * vectors
        earlier_rows = shifted(as_sent(scaled), "vox", 1).astype(scaled.dtype)
        window_rows = jnp.concatenate([earlier_rows, scaled], axis=0)
        forward = product(local_graph, window_rows)
        returns = product(local_graph.T, scaled)
        arrived = shifted(as_sent(returns[:voxels_here]), "vox", -1)
        images = 0.5 * (
            vectors + scaling[:, None] * (scaled + forward + returns[voxels_here:] + arrived)
        )
        vectors = orthonormal(images)
    return vectors


def solution(mesh):
    placed = (P("subj", "vox", None), P("vox"), P("vox", None), P("vox", None))
    return jax.shard_map(
        on_device, mesh=mesh, in_specs=placed, out_specs=P("vox", None), check_vma=False
    )
```

```python
import functools
import math

import jax
import jax.numpy as jnp
from jax import lax
from jax.experimental import pallas as pl
from jax.experimental.pallas import tpu as pltpu
from jax.sharding import PartitionSpec as P

ITERS = 3
REACH = 2
WELL_CONDITIONED = 64.0


NT = (((1,), (1,)), ((), ()))
NN = (((1,), (0,)), ((), ()))
VMEM = pl.BlockSpec(memory_space=pltpu.VMEM)


def dot(left, right, dims=NN, precision=None):
    return lax.dot_general(
        left, right, dims, precision=precision, preferred_element_type=jnp.float32
    )


def exchanged(value, axis, distance):
    count = lax.axis_size(axis)
    return lax.ppermute(value, axis, [(i, i ^ distance) for i in range(count)])


def summed_over(value, axis):
    count = lax.axis_size(axis)
    if count & (count - 1):
        return lax.psum(value, axis)
    stride = 1
    while stride < count:
        if stride > 1 and 4 * stride <= count:
            first, second, third = (exchanged(value, axis, k * stride) for k in (1, 2, 3))
            value = (value + first) + (second + third)
            stride *= 4
        else:
            value = value + exchanged(value, axis, stride)
            stride *= 2
    return value


def shifted(shard, axis, by):
    count = lax.axis_size(axis)
    pairs = [(i, i + by) for i in range(count) if 0 <= i + by < count]
    return lax.ppermute(shard, axis, pairs)


def standardize(z_ref, s, series_ref, q):
    width = series_ref.shape[1]
    for start in range(0, width, 32):
        values = series_ref[q, start : start + 32, :].astype(jnp.float32)
        center = values - jnp.mean(values, axis=-1, keepdims=True)
        spread = jnp.mean(center * center, axis=-1, keepdims=True)
        z_ref[s, start : start + 32, :] = (center * lax.rsqrt(spread + 1e-05)).astype(jnp.bfloat16)


def picked_sums(corr_ref, marks_ref, first_mark, offsets):
    slots, width = corr_ref.shape
    marks = [jnp.broadcast_to(marks_ref[k : k + 1, :], (8, width)) for k in range(offsets)]
    row = lax.broadcasted_iota(jnp.int32, (8, width), 0) + first_mark
    sums = [jnp.zeros((8, width), jnp.float32) for _ in range(offsets)]
    for start in range(0, slots, 8):
        values = corr_ref[start : start + 8, :]
        for k in range(offsets):
            sums[k] = sums[k] + jnp.where(marks[k] == row + start, values, 0.0)
    return [jnp.sum(s, axis=0, keepdims=True) for s in sums]


def own_kernel(offsets, series_ref, marks_ref, z_ref, sums_ref, corr_ref):
    subjects, width, _ = series_ref.shape
    total = None
    for s in range(subjects):
        standardize(z_ref, s, series_ref, s)
        part = dot(z_ref[s], z_ref[s], NT)
        total = part if total is None else total + part
    corr_ref[...] = total
    sums_ref[...] = jnp.zeros_like(sums_ref)
    for k, row in enumerate(picked_sums(corr_ref, marks_ref, width + 1, offsets)):
        sums_ref[k : k + 1, :] = row


def first_earlier_kernel(series_ref, z_ref, corr_ref, zs_ref):
    subjects = series_ref.shape[0]
    total = None
    for s in range(subjects):
        standardize(zs_ref, s, series_ref, s)
        part = dot(zs_ref[s], z_ref[s], NT)
        total = part if total is None else total + part
    corr_ref[...] = total


def last_earlier_kernel(
    offsets, series_ref, z_ref, marks_ref, own_ref, before_ref, sums_ref, zs_ref, corr_ref
):
    subjects = series_ref.shape[0]
    skip = z_ref.shape[0] - subjects
    total = before_ref[...]
    for s in range(subjects):
        standardize(zs_ref, s, series_ref, s)
        total = total + dot(zs_ref[s], z_ref[skip + s], NT)
    corr_ref[...] = total
    sums_ref[...] = own_ref[...]
    for k, row in enumerate(picked_sums(corr_ref, marks_ref, 1, offsets)):
        sums_ref[k : k + 1, :] += row


def chosen(flag, yes, no):
    return jnp.where(flag, yes, no)


def around(flags_ref, own, one, two, three, four):
    odd, high = flags_ref[1] == 1, flags_ref[2] == 1
    return [
        chosen(high, three, four),
        chosen(odd, one, two),
        own,
        chosen(odd, two, one),
        chosen(high, four, three),
    ]


def own_data_kernel(vectors_ref, neighbours_ref, live_ref, data_ref, marks_ref):
    vecs = vectors_ref.shape[0]
    offsets, width = neighbours_ref.shape
    living = live_ref[...].astype(jnp.float32)
    marks = neighbours_ref[...] + 1
    marks_ref[...] = marks
    data_ref[...] = jnp.zeros_like(data_ref)
    data_ref[:vecs, :] = vectors_ref[...] * living
    data_ref[vecs : vecs + offsets, :] = marks.astype(jnp.float32)
    data_ref[vecs + offsets : vecs + offsets + 1, :] = living


def stack_kernel(flags_ref, own_ref, one_ref, two_ref, three_ref, four_ref, stack_ref):
    parts = (own_ref, one_ref, two_ref, three_ref, four_ref)
    for i, part in enumerate(around(flags_ref, *(r[...] for r in parts))):
        stack_ref[i] = part


def window_kernel(
    offsets, vecs, flags_ref, same_ref, other_ref, vec_ref, live_ref, which_ref, marks_ref
):
    width = same_ref.shape[2]
    lists = 2 * REACH + 4
    nrows = marks_ref.shape[1]
    core = flags_ref[0]
    for a in range(lists):
        if a % 2:
            data = same_ref[(a - 3) // 2 + REACH]
        else:
            data = other_ref[(a - 4) // 2 + REACH + core]
        marks_ref[a] = data[vecs:, :].astype(jnp.int32)
        if a < lists - 1:
            vec_ref[a] = data[:vecs, :]
            live_ref[a] = jnp.broadcast_to(
                data[vecs + offsets : vecs + offsets + 1, :], (8, width)
            )
    chunk = 64
    base = lax.broadcasted_iota(jnp.int32, (chunk, width), 0) + 1

    def dense(step, carry):
        a = step // (width // chunk)
        start = pl.multiple_of((step % (width // chunk)) * chunk, chunk)
        for side in (0, 1):
            rows = base + (start + (1 - side) * width)
            value = jnp.full((chunk, width), nrows - 1, jnp.int32)
            for k in range(offsets):
                value = jnp.where(marks_ref[a + side, k : k + 1, :] == rows, k, value)
            which_ref[2 * a + side, pl.ds(start, chunk), :] = value
        return carry

    lax.fori_loop(0, (lists - 1) * (width // chunk), dense, 0)


def graph_kernel(offsets, scale, flags_ref, *refs):
    pairs = refs[:5]
    vec_ref, live_ref, which_ref, marks_ref = refs[5:9]
    y_ref, gram_ref = refs[9:11]
    hi_ref, lo_ref, weight_ref, scale_ref, block_ref = refs[11:]
    vecs, width = y_ref.shape
    lists = 2 * REACH + 4
    nrows = marks_ref.shape[1]
    core = flags_ref[0]
    same = around(flags_ref, *(r[0] for r in pairs))
    other = around(flags_ref, *(r[1] for r in pairs))
    listed = lax.broadcasted_iota(jnp.int32, (nrows, width), 0) < offsets
    for a in range(lists):
        if a % 2:
            sums = same[(a - 3) // 2 + REACH]
        else:
            i = (a - 4) // 2 + REACH
            sums = chosen(core == 1, other[i + 1], other[i])
        present = jnp.logical_and(listed, marks_ref[a] > 0)
        weight_ref[a] = jnp.where(present, jnp.exp(scale * sums), 0.0)

    def split(a, first, value):
        high = value.astype(jnp.bfloat16)
        hi_ref[a, first : first + width, :] = high
        lo_ref[a, first : first + width, :] = (value - high.astype(jnp.float32)).astype(
            jnp.bfloat16
        )

    def dense(a, carry):
        for side in (0, 1):
            for lane in range(0, width, 128):
                tables = [
                    weight_ref[a + side, g : g + 8, lane : lane + 128] for g in range(0, nrows, 8)
                ]
                for row in range(0, width, 8):
                    which = which_ref[2 * a + side, row : row + 8, lane : lane + 128]
                    low = jnp.bitwise_and(which, 7)
                    value = None
                    for g, table in enumerate(tables):
                        entry = jnp.take_along_axis(
                            table, low, axis=0, mode="promise_in_bounds"
                        )
                        value = entry if g == 0 else jnp.where(which >= 8 * g, entry, value)
                    block_ref[side, row : row + 8, lane : lane + 128] = value
        inside, before = block_ref[0], block_ref[1]
        inside_t, before_t = inside.T, before.T
        owed = jnp.sum(inside_t + before_t, axis=0, keepdims=True)
        degree = 1.0 + jnp.sum(weight_ref[a], axis=0, keepdims=True) + owed
        scale_ref[a] = live_ref[a] * lax.rsqrt(degree)
        split(a, width, inside + inside_t)
        split(a, 2 * width, before_t)
        split(a + 1, 0, before)
        return carry

    lax.fori_loop(0, lists - 1, dense, 0)

    scales = [scale_ref[a][0:1, :] for a in range(lists - 1)]
    vectors = {a: vec_ref[a] for a in range(lists - 1)}
    for step in range(ITERS):
        scaled, sent, short = {}, {}, {}
        for a in vectors:
            scaled[a] = scales[a] * vectors[a]
            short[a] = scaled[a].astype(jnp.bfloat16)
            low = (scaled[a] - short[a].astype(jnp.float32)).astype(jnp.bfloat16)
            sent[a] = jnp.concatenate([short[a], low], axis=0)
        images = {}
        for a in range(step + 1, lists - 2 - step):
            window = jnp.concatenate([sent[a - 1], sent[a], sent[a + 1]], axis=1)
            both = dot(window, hi_ref[a])
            near = dot(window[:vecs], lo_ref[a])
            edges = both[:vecs] + both[vecs:] + near
            images[a] = 0.5 * (vectors[a] + scales[a] * (scaled[a] + edges))
        vectors = images
    result = vectors[ITERS]
    y_ref[...] = result
    gram = dot(result, result, NT, lax.Precision.HIGHEST)
    half = vecs // 2
    gram_ref[...] = jnp.concatenate([gram[:half], gram[half:]], axis=1)


def factor_kernel(gram_ref, inverse_ref, bound_ref, work_ref):
    vecs = inverse_ref.shape[0]
    packed = gram_ref[...]
    gram = jnp.concatenate([packed[:, :vecs], packed[:, vecs:]], axis=0)
    row = lax.broadcasted_iota(jnp.int32, (vecs, vecs), 0)
    lane = lax.broadcasted_iota(jnp.int32, (vecs, vecs), 1)
    eye = (row == lane).astype(jnp.float32)
    full = jnp.concatenate([gram, eye], axis=1)
    blocks = [full[i : i + 8, :] for i in range(0, vecs, 8)]
    count = len(blocks)
    wide = 2 * vecs
    sub = lax.broadcasted_iota(jnp.int32, (8, wide), 0)
    for p in range(count):
        columns = [
            [jnp.broadcast_to(b[:, 8 * p + t : 8 * p + t + 1], (8, wide)) for b in blocks[p:]]
            for t in range(8)
        ]
        for t in range(8):
            pivot = jnp.broadcast_to(columns[t][0][t : t + 1, :], (8, wide))
            inverse = 1.0 / pivot
            line = jnp.broadcast_to(blocks[p][t : t + 1, :], (8, wide))
            j = 8 * p + t
            work_ref[j : j + 1, :] = (line * lax.rsqrt(pivot))[0:1, :]
            if j == vecs - 1:
                break
            times = [c * inverse for c in columns[t]]
            times[0] = jnp.where(sub > t, times[0], 0.0)
            later = [
                jnp.broadcast_to(columns[u][0][t : t + 1, :], (8, wide)) for u in range(t + 1, 8)
            ]
            for i in range(p, count):
                m = times[i - p]
                blocks[i] = blocks[i] - m * line
                for u in range(t + 1, 8):
                    columns[u][i - p] = columns[u][i - p] - m * later[u - t - 1]
    inverse_factor = work_ref[:, vecs:]
    diagonal = jnp.sum(gram * eye, axis=0, keepdims=True)
    bound_ref[0, 0] = jnp.sum(inverse_factor * inverse_factor * diagonal)
    inverse_ref[...] = inverse_factor


def solve_kernel(inverse_ref, y_ref, x_ref):
    x_ref[...] = dot(inverse_ref[...], y_ref[...], NN, lax.Precision.HIGHEST)


def dense_graph(weight, slots, columns_total):
    column_ids = jnp.arange(columns_total, dtype=jnp.int32)
    matrix = jnp.zeros((weight.shape[0], columns_total), jnp.float32)
    for offset in range(weight.shape[1]):
        hits = (slots[:, offset][:, None] == column_ids[None, :]).astype(jnp.float32)
        matrix = matrix + weight[:, offset][:, None] * hits
    return matrix


def product(left, right):
    return jnp.dot(left, right, precision=lax.Precision.HIGHEST)


def step_by_step(summed, scale, live_mask, neighbours, start_vectors):
    voxels_here = start_vectors.shape[0]
    weight = jnp.where(neighbours >= 0, jnp.exp(scale * summed), 0.0)
    living = live_mask.astype(jnp.float32)
    local_graph = dense_graph(weight, neighbours, 2 * voxels_here)
    owed = jnp.sum(local_graph, axis=0)
    received = shifted(owed[:voxels_here], "vox", -1)
    degree = 1.0 + jnp.sum(weight, axis=1) + owed[voxels_here:] + received
    scaling = living * lax.rsqrt(degree)
    vectors = living[:, None] * start_vectors

    def once(_, vectors):
        scaled = scaling[:, None] * vectors
        earlier_rows = shifted(scaled, "vox", 1)
        window_rows = jnp.concatenate([earlier_rows, scaled], axis=0)
        forward = product(local_graph, window_rows)
        returns = product(local_graph.T, scaled)
        arrived = shifted(returns[:voxels_here], "vox", -1)
        images = 0.5 * (
            vectors + scaling[:, None] * (scaled + forward + returns[voxels_here:] + arrived)
        )
        gram_matrix = summed_over(product(images.T, images), "vox")
        factor = jnp.linalg.cholesky(gram_matrix)
        return lax.linalg.triangular_solve(
            factor, images, left_side=False, lower=True, transpose_a=True
        )

    return lax.fori_loop(0, ITERS, once, vectors)


def call(kernel, outs, *args, scratch=(), out_specs=None, first=VMEM, flops=1_000_000, vmem=16):
    return pl.pallas_call(
        kernel,
        out_shape=outs,
        in_specs=[first] + [VMEM] * (len(args) - 1),
        out_specs=out_specs or jax.tree.map(lambda _: VMEM, outs),
        scratch_shapes=list(scratch),
        cost_estimate=pl.CostEstimate(flops=flops, bytes_accessed=1 << 18, transcendentals=0),
        compiler_params=pltpu.CompilerParams(vmem_limit_bytes=vmem << 20),
    )(*args)


def neighbour_exchanges(value):
    count = lax.axis_size("vox")
    found = []
    for distance in (2, 4):
        for late in (0, distance):
            pairs = [(i, ((i + late) ^ distance) - late) for i in range(count)]
            pairs = [(i, j) for i, j in pairs if 0 <= j < count]
            found.append(lax.ppermute(value, "vox", pairs))
    return found


def on_device(series, live_mask, neighbours, start_vectors):
    subjects, width, frames = series.shape
    offsets = neighbours.shape[1]
    vecs = start_vectors.shape[1]
    shape = jax.ShapeDtypeStruct
    f32 = jnp.float32
    groups = lax.axis_size("subj")
    scale = 0.5 / math.sqrt(frames * subjects * groups)
    rows = -(-(offsets + 1) // 8) * 8
    lists = 2 * REACH + 4
    smem = pl.BlockSpec(memory_space=pltpu.SMEM)
    place = lax.axis_index("vox").astype(jnp.int32)
    flags = jnp.stack([place % 2, (place // 2) % 2, (place // 4) % 2])
    square = pltpu.VMEM((width, width), f32)

    cut = subjects // 2
    with jax.named_scope("shift_one"):
        arriving_first = shifted(series[:cut], "vox", 1)
    with jax.named_scope("shift_two"):
        arriving_last = shifted(series[cut:], "vox", 1)

    data, marks = call(
        own_data_kernel,
        (shape((vecs + rows, width), f32), shape((offsets, width), jnp.int32)),
        start_vectors.T,
        neighbours.T,
        live_mask[None, :],
    )
    with jax.named_scope("data_around"):
        data_around = neighbour_exchanges(data)
    data_same = call(
        stack_kernel,
        shape((5, vecs + rows, width), f32),
        flags,
        data,
        *data_around,
        first=smem,
    )
    with jax.named_scope("data_core"):
        data_other = exchanged(data_same, "vox", 1)
    window = call(
        functools.partial(window_kernel, offsets, vecs),
        (
            shape((lists - 1, vecs, width), f32),
            shape((lists - 1, 8, width), f32),
            shape((2 * (lists - 1), width, width), jnp.int32),
            shape((lists, rows, width), jnp.int32),
        ),
        flags,
        data_same,
        data_other,
        first=smem,
    )

    z, own = call(
        functools.partial(own_kernel, offsets),
        (shape(series.shape, jnp.bfloat16), shape((rows, width), f32)),
        series,
        marks,
        scratch=[square],
    )
    corr = call(
        first_earlier_kernel,
        shape((width, width), f32),
        arriving_first,
        z,
        scratch=[pltpu.VMEM((cut, width, frames), jnp.bfloat16)],
    )
    partial_sums = call(
        functools.partial(last_earlier_kernel, offsets),
        shape((rows, width), f32),
        arriving_last,
        z,
        marks,
        own,
        corr,
        scratch=[pltpu.VMEM((subjects - cut, width, frames), jnp.bfloat16), square],
    )

    if groups == 2:
        both = ("vox", "subj")
        with jax.named_scope("sums_subj"):
            opposite = exchanged(partial_sums, "subj", 1)
        with jax.named_scope("sums_core"):
            beside = exchanged(partial_sums, "vox", 1)
        with jax.named_scope("sums_cross"):
            across = exchanged(partial_sums, both, 3)
        pair = jnp.stack([partial_sums + opposite, beside + across])
    else:
        summed = summed_over(partial_sums, "subj")
        pair = jnp.stack([summed, exchanged(summed, "vox", 1)])
    with jax.named_scope("sums_around"):
        pairs_around = neighbour_exchanges(pair)

    y, gram = call(
        functools.partial(graph_kernel, offsets, scale),
        (shape((vecs, width), f32), shape((vecs // 2, 2 * vecs), f32)),
        flags,
        pair,
        *pairs_around,
        *window,
        scratch=[
            pltpu.VMEM((lists, 3 * width, width), jnp.bfloat16),
            pltpu.VMEM((lists, 3 * width, width), jnp.bfloat16),
            pltpu.VMEM((lists, rows, width), f32),
            pltpu.VMEM((lists, 8, width), f32),
            pltpu.VMEM((2, width, width), f32),
        ],
        first=smem,
    )
    gram = summed_over(gram, "vox")
    inverse_factor, bound = call(
        factor_kernel,
        (shape((vecs, vecs), f32), shape((1, 1), f32)),
        gram,
        out_specs=(VMEM, smem),
        scratch=[pltpu.VMEM((vecs, 2 * vecs), f32)],
    )
    return lax.cond(
        bound[0, 0] <= WELL_CONDITIONED * vecs,
        lambda: call(solve_kernel, shape((vecs, width), f32), inverse_factor, y).T,
        lambda: step_by_step(
            pair[0, :offsets].T, scale, live_mask, neighbours, start_vectors
        ),
    )


def solution(mesh):
    placed = (P("subj", "vox", None), P("vox"), P("vox", None), P("vox", None))
    return jax.shard_map(
        on_device, mesh=mesh, in_specs=placed, out_specs=P("vox", None), check_vma=False
    )
```

```python
import functools
import math

import jax
import jax.numpy as jnp
from jax import lax
from jax.experimental import pallas as pl
from jax.experimental.pallas import tpu as pltpu
from jax.sharding import PartitionSpec as P


ITERS = 3
UNIT = 4
WELL_CONDITIONED = 64.0


NT = (((1,), (1,)), ((), ()))
NN = (((1,), (0,)), ((), ()))
VMEM = pl.BlockSpec(memory_space=pltpu.VMEM)


def dot(left, right, dims=NN, precision=None):
    return lax.dot_general(
        left, right, dims, precision=precision, preferred_element_type=jnp.float32
    )


def exchanged(value, axis, distance):
    count = lax.axis_size(axis)
    return lax.ppermute(value, axis, [(i, i ^ distance) for i in range(count)])


def summed_over(value, axis, stride=1):
    count = lax.axis_size(axis)
    if count & (count - 1):
        return lax.psum(value, axis) / stride
    while stride < count:
        if stride > 1 and 4 * stride <= count:
            first, second, third = (exchanged(value, axis, k * stride) for k in (1, 2, 3))
            value = (value + first) + (second + third)
            stride *= 4
        else:
            value = value + exchanged(value, axis, stride)
            stride *= 2
    return value


def shifted(shard, axis, by):
    count = lax.axis_size(axis)
    pairs = [(i, i + by) for i in range(count) if 0 <= i + by < count]
    return lax.ppermute(shard, axis, pairs)


def standardize(z_ref, s, series_ref, q):
    width = series_ref.shape[1]
    for start in range(0, width, 32):
        values = series_ref[q, start : start + 32, :].astype(jnp.float32)
        center = values - jnp.mean(values, axis=-1, keepdims=True)
        spread = jnp.mean(center * center, axis=-1, keepdims=True)
        z_ref[s, start : start + 32, :] = (center * lax.rsqrt(spread + 1e-05)).astype(jnp.bfloat16)


def picked_sums(corr_ref, marks_ref, first_mark, offsets):
    slots, width = corr_ref.shape
    marks = [jnp.broadcast_to(marks_ref[k : k + 1, :], (8, width)) for k in range(offsets)]
    row = lax.broadcasted_iota(jnp.int32, (8, width), 0) + first_mark
    sums = [jnp.zeros((8, width), jnp.float32) for _ in range(offsets)]
    for start in range(0, slots, 8):
        values = corr_ref[start : start + 8, :]
        for k in range(offsets):
            sums[k] = sums[k] + jnp.where(marks[k] == row + start, values, 0.0)
    return [jnp.sum(s, axis=0, keepdims=True) for s in sums]


def own_kernel(offsets, series_ref, marks_ref, z_ref, sums_ref, corr_ref):
    subjects, width, _ = series_ref.shape
    total = None
    for s in range(subjects):
        standardize(z_ref, s, series_ref, s)
        part = dot(z_ref[s], z_ref[s], NT)
        total = part if total is None else total + part
    corr_ref[...] = total
    sums_ref[...] = jnp.zeros_like(sums_ref)
    for k, row in enumerate(picked_sums(corr_ref, marks_ref, width + 1, offsets)):
        sums_ref[k : k + 1, :] = row


def earlier_kernel(offsets, series_ref, z_ref, marks_ref, own_ref, sums_ref, zs_ref, corr_ref):
    subjects = series_ref.shape[0]
    total = None
    for s in range(subjects):
        standardize(zs_ref, s, series_ref, s)
        part = dot(zs_ref[s], z_ref[s], NT)
        total = part if total is None else total + part
    corr_ref[...] = total
    sums_ref[...] = own_ref[...]
    for k, row in enumerate(picked_sums(corr_ref, marks_ref, 1, offsets)):
        sums_ref[k : k + 1, :] += row


def chosen(flag, yes, no):
    return jnp.where(flag, yes, no)


def in_order(flags_ref, own, three, four):
    odd = flags_ref[1] == 1
    return chosen(odd, three, four), own, chosen(odd, four, three)


def own_data_kernel(vectors_ref, neighbours_ref, live_ref, data_ref, marks_ref):
    vecs = vectors_ref.shape[0]
    offsets, _ = neighbours_ref.shape
    living = live_ref[...].astype(jnp.float32)
    marks = neighbours_ref[...] + 1
    marks_ref[...] = marks
    data_ref[...] = jnp.zeros_like(data_ref)
    data_ref[:vecs, :] = vectors_ref[...] * living
    data_ref[vecs : vecs + offsets, :] = marks.astype(jnp.float32)
    data_ref[vecs + offsets : vecs + offsets + 1, :] = living


def compact_kernel(vecs, data_ref, partner_ref, row_ref):
    for j, ref in enumerate((data_ref, partner_ref)):
        marks = ref[vecs:, :].astype(jnp.int32)
        digits = jnp.concatenate([marks // 16, marks % 16], axis=0)
        row_ref[j, :vecs, :] = ref[:vecs, :].astype(jnp.bfloat16)
        row_ref[j, vecs:, :] = digits.astype(jnp.float32).astype(jnp.bfloat16)


def stack_kernel(vecs, flags_ref, data_ref, partner_ref, three_ref, four_ref, stack_ref):
    nrows = data_ref.shape[0] - vecs
    for j, ref in enumerate((data_ref, partner_ref)):
        parts = in_order(flags_ref, ref[...], three_ref[j], four_ref[j])
        for w, part in enumerate(parts):
            part = part.astype(jnp.float32)
            stack_ref[2 * w + j, :vecs, :] = part[:vecs]
            marks = part[vecs:]
            if w != 1:
                marks = 16.0 * marks[:nrows] + marks[nrows:]
            stack_ref[2 * w + j, vecs:, :] = marks


def find_entries(offsets, vecs, place, data_ref, which_ref, marks_ref):
    width = data_ref.shape[2]
    nrows = marks_ref.shape[1]
    for i in range(data_ref.shape[0]):
        marks_ref[i] = data_ref[i, vecs:, :].astype(jnp.int32)
    chunk = 128
    pieces = width // chunk
    base = lax.broadcasted_iota(jnp.int32, (chunk, width), 0) + (width + 1)

    def dense(step, carry):
        i = step // pieces
        start = pl.multiple_of((step % pieces) * chunk, chunk)
        rows = base + start
        value = jnp.full((chunk, width), nrows - 1, jnp.int32)
        for k in range(offsets):
            value = jnp.where(marks_ref[i, k : k + 1, :] == rows, k, value)
        b = UNIT * (i // 2) + lax.bitwise_xor(place, 2 * (i % 2))
        which_ref[b, pl.ds(start, chunk), :] = value
        return carry

    lax.fori_loop(0, data_ref.shape[0] * pieces, dense, 0)


def same_window_kernel(offsets, vecs, flags_ref, same_ref, which_ref, marks_ref):
    find_entries(offsets, vecs, flags_ref[0], same_ref, which_ref, marks_ref)


def other_window_kernel(
    offsets, vecs, flags_ref, same_ref, other_ref, _, which_ref, vec_ref, row_ref, marks_ref
):
    place = flags_ref[0]
    for i in range(same_ref.shape[0]):
        for ref, lift in ((same_ref, 0), (other_ref, 1)):
            b = UNIT * (i // 2) + lax.bitwise_xor(place, 2 * (i % 2) + lift)
            vec_ref[b] = ref[i, :vecs, :]
            row_ref[b] = ref[i, vecs:, :]
    find_entries(offsets, vecs, lax.bitwise_xor(place, 1), other_ref, which_ref, marks_ref)


def graph_kernel(offsets, flags_ref, *refs):
    row_ref, three_ref, four_ref = refs[:3]
    which_ref, vec_ref, data_ref = refs[3:6]
    y_ref, gram_ref = refs[6:8]
    graph_ref, weight_ref, mark_ref, scale_ref = refs[8:]
    vecs, width = y_ref.shape
    count, nrows = weight_ref.shape[:2]
    place = flags_ref[0]
    for r in range(UNIT):
        weights = in_order(flags_ref, row_ref[r], three_ref[r], four_ref[r])
        for w in range(3):
            b = UNIT * w + lax.bitwise_xor(place, r)
            weight_ref[b] = weights[w].astype(jnp.float32)
            mark_ref[b] = data_ref[b].astype(jnp.int32)

    chunk = 64
    base = lax.broadcasted_iota(jnp.int32, (chunk, width), 0) + 1

    def dense(b, carry):
        for lane in range(0, width, 128):
            tables = [weight_ref[b, g : g + 8, lane : lane + 128] for g in range(0, nrows, 8)]
            for row in range(0, width, 16):
                halves = []
                for start in (row, row + 8):
                    which = which_ref[b, start : start + 8, lane : lane + 128]
                    low = jnp.bitwise_and(which, 7)
                    value = None
                    for g, table in enumerate(tables):
                        entry = jnp.take_along_axis(table, low, axis=0, mode="promise_in_bounds")
                        value = entry if g == 0 else jnp.where(which >= 8 * g, entry, value)
                    halves.append(value)
                graph_ref[b, width + row : width + row + 16, lane : lane + 128] = jnp.concatenate(
                    halves, axis=0
                ).astype(jnp.bfloat16)
        for start in range(0, width, chunk):
            value = jnp.zeros((chunk, width), jnp.float32)
            for k in range(offsets):
                value = jnp.where(
                    mark_ref[b + 1, k : k + 1, :] == base + start,
                    weight_ref[b + 1, k : k + 1, :],
                    value,
                )
            graph_ref[b + 1, start : start + chunk, :] = value.astype(jnp.bfloat16)
        inside = graph_ref[b, width : 2 * width, :]
        inside_t, after = inside.T, graph_ref[b + 1, :width, :].T
        graph_ref[b, width : 2 * width, :] = inside + inside_t
        graph_ref[b, 2 * width :, :] = after
        owed = jnp.sum(inside_t.astype(jnp.float32) + after.astype(jnp.float32), axis=0)
        degree = 1.0 + jnp.sum(weight_ref[b], axis=0, keepdims=True) + owed[None, :]
        live = data_ref[b, offsets : offsets + 1, :]
        scale_ref[b] = jnp.broadcast_to(live * lax.rsqrt(degree), scale_ref.shape[1:])
        return carry

    lax.fori_loop(1, count - 1, dense, 0)

    scales = {b: scale_ref[b, 0:1, :] for b in range(1, count - 1)}
    vectors = {b: vec_ref[b] for b in range(1, count - 1)}
    for step in range(ITERS):
        scaled, sent = {}, {}
        for b in vectors:
            scaled[b] = scales[b] * vectors[b]
            high = scaled[b].astype(jnp.bfloat16)
            low = (scaled[b] - high.astype(jnp.float32)).astype(jnp.bfloat16)
            sent[b] = jnp.concatenate([high, low], axis=0)
        images = {}
        for b in range(step + 2, count - 2 - step):
            window = jnp.concatenate([sent[b - 1], sent[b], sent[b + 1]], axis=1)
            both = dot(window, graph_ref[b])
            edges = both[:vecs] + both[vecs:]
            images[b] = 0.5 * (vectors[b] + scales[b] * (scaled[b] + edges))
        vectors = images
    ours = [vectors[UNIT + r] for r in range(UNIT)]
    y = ours[0]
    for r in range(1, UNIT):
        y = chosen(place == r, ours[r], y)
    y_ref[...] = y
    joined = jnp.concatenate(ours, axis=1)
    gram = dot(joined, joined, NT, lax.Precision.HIGHEST)
    half = vecs // 2
    gram_ref[...] = jnp.concatenate([gram[:half], gram[half:]], axis=1)


def factor_kernel(gram_ref, inverse_ref, bound_ref, work_ref):
    vecs = inverse_ref.shape[0]
    packed = gram_ref[...]
    gram = jnp.concatenate([packed[:, :vecs], packed[:, vecs:]], axis=0)
    row = lax.broadcasted_iota(jnp.int32, (vecs, vecs), 0)
    lane = lax.broadcasted_iota(jnp.int32, (vecs, vecs), 1)
    eye = (row == lane).astype(jnp.float32)
    full = jnp.concatenate([gram, eye], axis=1)
    blocks = [full[i : i + 8, :] for i in range(0, vecs, 8)]
    count = len(blocks)
    wide = 2 * vecs
    sub = lax.broadcasted_iota(jnp.int32, (8, wide), 0)
    for p in range(count):
        columns = [
            [jnp.broadcast_to(b[:, 8 * p + t : 8 * p + t + 1], (8, wide)) for b in blocks[p:]]
            for t in range(8)
        ]
        for t in range(8):
            pivot = jnp.broadcast_to(columns[t][0][t : t + 1, :], (8, wide))
            inverse = 1.0 / pivot
            line = jnp.broadcast_to(blocks[p][t : t + 1, :], (8, wide))
            j = 8 * p + t
            work_ref[j : j + 1, :] = (line * lax.rsqrt(pivot))[0:1, :]
            if j == vecs - 1:
                break
            times = [c * inverse for c in columns[t]]
            times[0] = jnp.where(sub > t, times[0], 0.0)
            later = [
                jnp.broadcast_to(columns[u][0][t : t + 1, :], (8, wide)) for u in range(t + 1, 8)
            ]
            for i in range(p, count):
                m = times[i - p]
                blocks[i] = blocks[i] - m * line
                for u in range(t + 1, 8):
                    columns[u][i - p] = columns[u][i - p] - m * later[u - t - 1]
    inverse_factor = work_ref[:, vecs:]
    diagonal = jnp.sum(gram * eye, axis=0, keepdims=True)
    bound_ref[0, 0] = jnp.sum(inverse_factor * inverse_factor * diagonal)
    inverse_ref[...] = inverse_factor


def solve_kernel(inverse_ref, y_ref, x_ref):
    x_ref[...] = dot(inverse_ref[...], y_ref[...], NN, lax.Precision.HIGHEST)


def dense_graph(weight, slots, columns_total):
    column_ids = jnp.arange(columns_total, dtype=jnp.int32)
    matrix = jnp.zeros((weight.shape[0], columns_total), jnp.float32)
    for offset in range(weight.shape[1]):
        hits = (slots[:, offset][:, None] == column_ids[None, :]).astype(jnp.float32)
        matrix = matrix + weight[:, offset][:, None] * hits
    return matrix


def product(left, right):
    return jnp.dot(left, right, precision=lax.Precision.HIGHEST)


def step_by_step(summed, scale, live_mask, neighbours, start_vectors):
    voxels_here = start_vectors.shape[0]
    weight = jnp.where(neighbours >= 0, jnp.exp(scale * summed), 0.0)
    living = live_mask.astype(jnp.float32)
    local_graph = dense_graph(weight, neighbours, 2 * voxels_here)
    owed = jnp.sum(local_graph, axis=0)
    received = shifted(owed[:voxels_here], "vox", -1)
    degree = 1.0 + jnp.sum(weight, axis=1) + owed[voxels_here:] + received
    scaling = living * lax.rsqrt(degree)
    vectors = living[:, None] * start_vectors

    def once(_, vectors):
        scaled = scaling[:, None] * vectors
        earlier_rows = shifted(scaled, "vox", 1)
        window_rows = jnp.concatenate([earlier_rows, scaled], axis=0)
        forward = product(local_graph, window_rows)
        returns = product(local_graph.T, scaled)
        arrived = shifted(returns[:voxels_here], "vox", -1)
        images = 0.5 * (
            vectors + scaling[:, None] * (scaled + forward + returns[voxels_here:] + arrived)
        )
        gram_matrix = summed_over(product(images.T, images), "vox")
        factor = jnp.linalg.cholesky(gram_matrix)
        return lax.linalg.triangular_solve(
            factor, images, left_side=False, lower=True, transpose_a=True
        )

    return lax.fori_loop(0, ITERS, once, vectors)


def call(kernel, outs, *args, scratch=(), out_specs=None, first=VMEM, vmem=16, aliases=None):
    return pl.pallas_call(
        kernel,
        out_shape=outs,
        in_specs=[first] + [VMEM] * (len(args) - 1),
        out_specs=out_specs or jax.tree.map(lambda _: VMEM, outs),
        scratch_shapes=list(scratch),
        cost_estimate=pl.CostEstimate(flops=1_000_000, bytes_accessed=1 << 18, transcendentals=0),
        input_output_aliases=aliases or {},
        compiler_params=pltpu.CompilerParams(vmem_limit_bytes=vmem << 20),
    )(*args)


def pairwise(value, distance, late):
    count = lax.axis_size("vox")
    pairs = [(i, ((i + late) ^ distance) - late) for i in range(count)]
    return lax.ppermute(value, "vox", [(i, j) for i, j in pairs if 0 <= j < count])


def on_device(series, live_mask, neighbours, start_vectors):
    subjects, width, frames = series.shape
    offsets = neighbours.shape[1]
    vecs = start_vectors.shape[1]
    shape = jax.ShapeDtypeStruct
    f32 = jnp.float32
    groups = lax.axis_size("subj")
    scale = 0.5 / math.sqrt(frames * subjects * groups)
    rows = -(-(offsets + 1) // 8) * 8
    smem = pl.BlockSpec(memory_space=pltpu.SMEM)
    number = lax.axis_index("vox").astype(jnp.int32)
    flags = jnp.stack([number % UNIT, (number // UNIT) % 2])
    square = pltpu.VMEM((width, width), f32)

    arriving = shifted(series, "vox", 1)

    data, marks = call(
        own_data_kernel,
        (shape((vecs + rows, width), f32), shape((offsets, width), jnp.int32)),
        start_vectors.T,
        neighbours.T,
        live_mask[None, :],
    )
    data_partner = exchanged(data, "vox", 2)
    data_row = call(
        functools.partial(compact_kernel, vecs),
        shape((2, vecs + 2 * rows, width), jnp.bfloat16),
        data,
        data_partner,
    )
    data_rows = [pairwise(data_row, UNIT, late) for late in (0, UNIT)]
    data_same = call(
        functools.partial(stack_kernel, vecs),
        shape((6, vecs + rows, width), f32),
        flags,
        data,
        data_partner,
        *data_rows,
        first=smem,
    )
    data_other = exchanged(data_same, "vox", 1)
    blocks = 3 * UNIT
    entries = shape((blocks, width, width), jnp.int32)
    marks_scratch = pltpu.VMEM((6, rows, width), jnp.int32)
    half_which = call(
        functools.partial(same_window_kernel, offsets, vecs),
        entries,
        flags,
        data_same,
        first=smem,
        scratch=[marks_scratch],
    )
    window = call(
        functools.partial(other_window_kernel, offsets, vecs),
        (entries, shape((blocks, vecs, width), f32), shape((blocks, rows, width), f32)),
        flags,
        data_same,
        data_other,
        half_which,
        first=smem,
        scratch=[marks_scratch],
        aliases={3: 0},
    )
    z, own = call(
        functools.partial(own_kernel, offsets),
        (shape(series.shape, jnp.bfloat16), shape((rows, width), f32)),
        series,
        marks,
        scratch=[square],
    )
    partial_sums = call(
        functools.partial(earlier_kernel, offsets),
        shape((rows, width), f32),
        arriving,
        z,
        marks,
        own,
        scratch=[pltpu.VMEM(series.shape, jnp.bfloat16), square],
    )

    summed = summed_over(partial_sums, "subj")
    listed = lax.broadcasted_iota(jnp.int32, summed.shape, 0) < offsets
    present = jnp.logical_and(listed, data[vecs:, :] > 0.5)
    weight = jnp.where(present, jnp.exp(scale * summed), 0.0).astype(jnp.bfloat16)
    near = [weight]
    for r in range(1, UNIT):
        near.append(exchanged(weight, "vox", r))
    row = jnp.stack(near)
    rows_around = [pairwise(row, UNIT, late) for late in (0, UNIT)]

    y, gram = call(
        functools.partial(graph_kernel, offsets),
        (shape((vecs, width), f32), shape((vecs // 2, 2 * vecs), f32)),
        flags,
        row,
        *rows_around,
        *window,
        scratch=[
            pltpu.VMEM((blocks, 3 * width, width), jnp.bfloat16),
            pltpu.VMEM((blocks, rows, width), f32),
            pltpu.VMEM((blocks, rows, width), jnp.int32),
            pltpu.VMEM((blocks, 8, width), f32),
        ],
        first=smem,
        vmem=24,
    )
    gram = summed_over(gram, "vox", UNIT)
    inverse_factor, bound = call(
        factor_kernel,
        (shape((vecs, vecs), f32), shape((1, 1), f32)),
        gram,
        out_specs=(VMEM, smem),
        scratch=[pltpu.VMEM((vecs, 2 * vecs), f32)],
    )
    return lax.cond(
        bound[0, 0] <= WELL_CONDITIONED * vecs,
        lambda: call(solve_kernel, shape((vecs, width), f32), inverse_factor, y).T,
        lambda: step_by_step(
            summed[:offsets].T, scale, live_mask, neighbours, start_vectors
        ),
    )


def solution(mesh):
    placed = (P("subj", "vox", None), P("vox"), P("vox", None), P("vox", None))
    return jax.shard_map(
        on_device, mesh=mesh, in_specs=placed, out_specs=P("vox", None), check_vma=False
    )
```

```python
import functools
import math

import jax
import jax.numpy as jnp
from jax import lax
from jax.experimental import pallas as pl
from jax.experimental.pallas import tpu as pltpu
from jax.sharding import PartitionSpec as P


ITERS = 3
UNIT = 4
WELL_CONDITIONED = 64.0


NT = (((1,), (1,)), ((), ()))
NN = (((1,), (0,)), ((), ()))
VMEM = pl.BlockSpec(memory_space=pltpu.VMEM)


def dot(left, right, dims=NN, precision=None):
    return lax.dot_general(
        left, right, dims, precision=precision, preferred_element_type=jnp.float32
    )


def exchanged(value, axis, distance):
    count = lax.axis_size(axis)
    return lax.ppermute(value, axis, [(i, i ^ distance) for i in range(count)])


def summed_over(value, axis, stride=1):
    count = lax.axis_size(axis)
    if count & (count - 1):
        return lax.psum(value, axis) / stride
    while stride < count:
        if stride > 1 and 4 * stride <= count:
            parts = []
            for k in (1, 2, 3):
                parts.append(exchanged(value, axis, k * stride))
            first, second, third = parts
            value = (value + first) + (second + third)
            stride *= 4
        else:
            value = value + exchanged(value, axis, stride)
            stride *= 2
    return value


def shifted(shard, axis, by):
    count = lax.axis_size(axis)
    pairs = [(i, i + by) for i in range(count) if 0 <= i + by < count]
    return lax.ppermute(shard, axis, pairs)


def standardize(z_ref, s, series_ref, q):
    width = series_ref.shape[1]
    for start in range(0, width, 32):
        values = series_ref[q, start : start + 32, :].astype(jnp.float32)
        center = values - jnp.mean(values, axis=-1, keepdims=True)
        spread = jnp.mean(center * center, axis=-1, keepdims=True)
        z_ref[s, start : start + 32, :] = (center * lax.rsqrt(spread + 1e-05)).astype(jnp.bfloat16)


def picked_sums(corr_ref, marks_ref, first_mark, offsets):
    slots, width = corr_ref.shape
    marks = [jnp.broadcast_to(marks_ref[k : k + 1, :], (8, width)) for k in range(offsets)]
    row = lax.broadcasted_iota(jnp.int32, (8, width), 0) + first_mark
    sums = [jnp.zeros((8, width), jnp.float32) for _ in range(offsets)]
    for start in range(0, slots, 8):
        values = corr_ref[start : start + 8, :]
        for k in range(offsets):
            sums[k] = sums[k] + jnp.where(marks[k] == row + start, values, 0.0)
    return [jnp.sum(s, axis=0, keepdims=True) for s in sums]


def own_kernel(offsets, series_ref, marks_ref, z_ref, sums_ref, corr_ref):
    subjects, width, _ = series_ref.shape
    total = None
    for s in range(subjects):
        standardize(z_ref, s, series_ref, s)
        part = dot(z_ref[s], z_ref[s], NT)
        total = part if total is None else total + part
    corr_ref[...] = total
    sums_ref[...] = jnp.zeros_like(sums_ref)
    for k, row in enumerate(picked_sums(corr_ref, marks_ref, width + 1, offsets)):
        sums_ref[k : k + 1, :] = row


def earlier_kernel(offsets, series_ref, z_ref, marks_ref, own_ref, sums_ref, zs_ref, corr_ref):
    subjects = series_ref.shape[0]
    total = None
    for s in range(subjects):
        standardize(zs_ref, s, series_ref, s)
        part = dot(zs_ref[s], z_ref[s], NT)
        total = part if total is None else total + part
    corr_ref[...] = total
    sums_ref[...] = own_ref[...]
    for k, row in enumerate(picked_sums(corr_ref, marks_ref, 1, offsets)):
        sums_ref[k : k + 1, :] += row


def chosen(flag, yes, no):
    return jnp.where(flag, yes, no)


def in_order(flags_ref, own, three, four):
    odd = flags_ref[1] == 1
    return chosen(odd, three, four), own, chosen(odd, four, three)


def own_data_kernel(vectors_ref, neighbours_ref, live_ref, data_ref, marks_ref):
    vecs = vectors_ref.shape[0]
    offsets, _ = neighbours_ref.shape
    living = live_ref[...].astype(jnp.float32)
    marks = neighbours_ref[...] + 1
    marks_ref[...] = marks
    data_ref[...] = jnp.zeros_like(data_ref)
    data_ref[:vecs, :] = vectors_ref[...] * living
    data_ref[vecs : vecs + offsets, :] = marks.astype(jnp.float32)
    data_ref[vecs + offsets : vecs + offsets + 1, :] = living


def compact_kernel(vecs, data_ref, partner_ref, row_ref):
    for j, ref in enumerate((data_ref, partner_ref)):
        marks = ref[vecs:, :].astype(jnp.int32)
        digits = jnp.concatenate([marks // 16, marks % 16], axis=0)
        row_ref[j, :vecs, :] = ref[:vecs, :].astype(jnp.bfloat16)
        row_ref[j, vecs:, :] = digits.astype(jnp.float32).astype(jnp.bfloat16)


def stack_kernel(vecs, flags_ref, data_ref, partner_ref, three_ref, four_ref, stack_ref):
    nrows = data_ref.shape[0] - vecs
    for j, ref in enumerate((data_ref, partner_ref)):
        parts = in_order(flags_ref, ref[...], three_ref[j], four_ref[j])
        for w, part in enumerate(parts):
            part = part.astype(jnp.float32)
            stack_ref[2 * w + j, :vecs, :] = part[:vecs]
            marks = part[vecs:]
            if w != 1:
                marks = 16.0 * marks[:nrows] + marks[nrows:]
            stack_ref[2 * w + j, vecs:, :] = marks


def find_entries(offsets, vecs, place, data_ref, which_ref, marks_ref):
    width = data_ref.shape[2]
    nrows = marks_ref.shape[1]
    for i in range(data_ref.shape[0]):
        marks_ref[i] = data_ref[i, vecs:, :].astype(jnp.int32)
    chunk = 128
    pieces = width // chunk
    base = lax.broadcasted_iota(jnp.int32, (chunk, width), 0) + (width + 1)

    def dense(step, carry):
        i = step // pieces
        start = pl.multiple_of((step % pieces) * chunk, chunk)
        rows = base + start
        value = jnp.full((chunk, width), nrows - 1, jnp.int32)
        for k in range(offsets):
            value = jnp.where(marks_ref[i, k : k + 1, :] == rows, k, value)
        b = UNIT * (i // 2) + lax.bitwise_xor(place, 2 * (i % 2))
        which_ref[b, pl.ds(start, chunk), :] = value
        return carry

    lax.fori_loop(0, data_ref.shape[0] * pieces, dense, 0)


def same_window_kernel(offsets, vecs, flags_ref, same_ref, which_ref, marks_ref):
    find_entries(offsets, vecs, flags_ref[0], same_ref, which_ref, marks_ref)


def other_window_kernel(
    offsets, vecs, flags_ref, same_ref, other_ref, _, which_ref, vec_ref, row_ref, marks_ref
):
    place = flags_ref[0]
    for i in range(same_ref.shape[0]):
        for ref, lift in ((same_ref, 0), (other_ref, 1)):
            b = UNIT * (i // 2) + lax.bitwise_xor(place, 2 * (i % 2) + lift)
            vec_ref[b] = ref[i, :vecs, :]
            row_ref[b] = ref[i, vecs:, :]
    find_entries(offsets, vecs, lax.bitwise_xor(place, 1), other_ref, which_ref, marks_ref)


def graph_kernel(offsets, flags_ref, *refs):
    row_ref, three_ref, four_ref = refs[:3]
    which_ref, vec_ref, data_ref = refs[3:6]
    y_ref, gram_ref = refs[6:8]
    graph_ref, weight_ref, mark_ref, scale_ref = refs[8:]
    vecs, width = y_ref.shape
    count, nrows = weight_ref.shape[:2]
    place = flags_ref[0]
    for r in range(UNIT):
        weights = in_order(flags_ref, row_ref[r], three_ref[r], four_ref[r])
        for w in range(3):
            b = UNIT * w + lax.bitwise_xor(place, r)
            weight_ref[b] = weights[w].astype(jnp.float32)
            mark_ref[b] = data_ref[b].astype(jnp.int32)

    chunk = 64
    base = lax.broadcasted_iota(jnp.int32, (chunk, width), 0) + 1

    def dense(b, carry):
        for lane in range(0, width, 128):
            tables = [weight_ref[b, g : g + 8, lane : lane + 128] for g in range(0, nrows, 8)]
            for row in range(0, width, 16):
                halves = []
                for start in (row, row + 8):
                    which = which_ref[b, start : start + 8, lane : lane + 128]
                    low = jnp.bitwise_and(which, 7)
                    value = None
                    for g, table in enumerate(tables):
                        entry = jnp.take_along_axis(table, low, axis=0, mode="promise_in_bounds")
                        value = entry if g == 0 else jnp.where(which >= 8 * g, entry, value)
                    halves.append(value)
                graph_ref[b, width + row : width + row + 16, lane : lane + 128] = jnp.concatenate(
                    halves, axis=0
                ).astype(jnp.bfloat16)
        for start in range(0, width, chunk):
            value = jnp.zeros((chunk, width), jnp.float32)
            for k in range(offsets):
                value = jnp.where(
                    mark_ref[b + 1, k : k + 1, :] == base + start,
                    weight_ref[b + 1, k : k + 1, :],
                    value,
                )
            graph_ref[b + 1, start : start + chunk, :] = value.astype(jnp.bfloat16)
        inside = graph_ref[b, width : 2 * width, :]
        inside_t, after = inside.T, graph_ref[b + 1, :width, :].T
        graph_ref[b, width : 2 * width, :] = inside + inside_t
        graph_ref[b, 2 * width :, :] = after
        owed = jnp.sum(inside_t.astype(jnp.float32) + after.astype(jnp.float32), axis=0)
        degree = 1.0 + jnp.sum(weight_ref[b], axis=0, keepdims=True) + owed[None, :]
        live = data_ref[b, offsets : offsets + 1, :]
        scale_ref[b] = jnp.broadcast_to(live * lax.rsqrt(degree), scale_ref.shape[1:])
        return carry

    lax.fori_loop(1, count - 1, dense, 0, unroll=2)

    scales = {b: scale_ref[b, 0:1, :] for b in range(1, count - 1)}
    vectors = {b: vec_ref[b] for b in range(1, count - 1)}
    for step in range(ITERS):
        scaled, sent = {}, {}
        for b in vectors:
            scaled[b] = scales[b] * vectors[b]
            high = scaled[b].astype(jnp.bfloat16)
            low = (scaled[b] - high.astype(jnp.float32)).astype(jnp.bfloat16)
            sent[b] = jnp.concatenate([high, low], axis=0)
        images = {}
        for b in range(step + 2, count - 2 - step):
            window = jnp.concatenate([sent[b - 1], sent[b], sent[b + 1]], axis=1)
            both = dot(window, graph_ref[b])
            edges = both[:vecs] + both[vecs:]
            images[b] = 0.5 * (vectors[b] + scales[b] * (scaled[b] + edges))
        vectors = images
    ours = [vectors[UNIT + r] for r in range(UNIT)]
    y = ours[0]
    for r in range(1, UNIT):
        y = chosen(place == r, ours[r], y)
    y_ref[...] = y
    joined = jnp.concatenate(ours, axis=1)
    gram = dot(joined, joined, NT, lax.Precision.HIGHEST)
    half = vecs // 2
    gram_ref[...] = jnp.concatenate([gram[:half], gram[half:]], axis=1)


def factor_kernel(gram_ref, inverse_ref, bound_ref, work_ref):
    vecs = inverse_ref.shape[0]
    packed = gram_ref[...]
    gram = jnp.concatenate([packed[:, :vecs], packed[:, vecs:]], axis=0)
    row = lax.broadcasted_iota(jnp.int32, (vecs, vecs), 0)
    lane = lax.broadcasted_iota(jnp.int32, (vecs, vecs), 1)
    eye = (row == lane).astype(jnp.float32)
    full = jnp.concatenate([gram, eye], axis=1)
    blocks = [full[i : i + 8, :] for i in range(0, vecs, 8)]
    count = len(blocks)
    wide = 2 * vecs
    sub = lax.broadcasted_iota(jnp.int32, (8, wide), 0)
    for p in range(count):
        columns = [
            [jnp.broadcast_to(b[:, 8 * p + t : 8 * p + t + 1], (8, wide)) for b in blocks[p:]]
            for t in range(8)
        ]
        for t in range(8):
            pivot = jnp.broadcast_to(columns[t][0][t : t + 1, :], (8, wide))
            inverse = 1.0 / pivot
            line = jnp.broadcast_to(blocks[p][t : t + 1, :], (8, wide))
            j = 8 * p + t
            work_ref[j : j + 1, :] = (line * lax.rsqrt(pivot))[0:1, :]
            if j == vecs - 1:
                break
            times = [c * inverse for c in columns[t]]
            times[0] = jnp.where(sub > t, times[0], 0.0)
            later = [
                jnp.broadcast_to(columns[u][0][t : t + 1, :], (8, wide)) for u in range(t + 1, 8)
            ]
            for i in range(p, count):
                m = times[i - p]
                blocks[i] = blocks[i] - m * line
                for u in range(t + 1, 8):
                    columns[u][i - p] = columns[u][i - p] - m * later[u - t - 1]
    inverse_factor = work_ref[:, vecs:]
    diagonal = jnp.sum(gram * eye, axis=0, keepdims=True)
    bound_ref[0, 0] = jnp.sum(inverse_factor * inverse_factor * diagonal)
    inverse_ref[...] = inverse_factor


def solve_kernel(inverse_ref, y_ref, x_ref):
    x_ref[...] = dot(inverse_ref[...], y_ref[...], NN, lax.Precision.HIGHEST)


def dense_graph(weight, slots, columns_total):
    column_ids = jnp.arange(columns_total, dtype=jnp.int32)
    matrix = jnp.zeros((weight.shape[0], columns_total), jnp.float32)
    for offset in range(weight.shape[1]):
        hits = (slots[:, offset][:, None] == column_ids[None, :]).astype(jnp.float32)
        matrix = matrix + weight[:, offset][:, None] * hits
    return matrix


def product(left, right):
    return jnp.dot(left, right, precision=lax.Precision.HIGHEST)


def step_by_step(summed, scale, live_mask, neighbours, start_vectors):
    voxels_here = start_vectors.shape[0]
    weight = jnp.where(neighbours >= 0, jnp.exp(scale * summed), 0.0)
    living = live_mask.astype(jnp.float32)
    local_graph = dense_graph(weight, neighbours, 2 * voxels_here)
    owed = jnp.sum(local_graph, axis=0)
    received = shifted(owed[:voxels_here], "vox", -1)
    degree = 1.0 + jnp.sum(weight, axis=1) + owed[voxels_here:] + received
    scaling = living * lax.rsqrt(degree)
    vectors = living[:, None] * start_vectors

    def once(_, vectors):
        scaled = scaling[:, None] * vectors
        earlier_rows = shifted(scaled, "vox", 1)
        window_rows = jnp.concatenate([earlier_rows, scaled], axis=0)
        forward = product(local_graph, window_rows)
        returns = product(local_graph.T, scaled)
        arrived = shifted(returns[:voxels_here], "vox", -1)
        images = 0.5 * (
            vectors + scaling[:, None] * (scaled + forward + returns[voxels_here:] + arrived)
        )
        gram_matrix = summed_over(product(images.T, images), "vox")
        factor = jnp.linalg.cholesky(gram_matrix)
        return lax.linalg.triangular_solve(
            factor, images, left_side=False, lower=True, transpose_a=True
        )

    return lax.fori_loop(0, ITERS, once, vectors)


def call(kernel, outs, *args, scratch=(), out_specs=None, first=VMEM, vmem=16, aliases=None):
    return pl.pallas_call(
        kernel,
        out_shape=outs,
        in_specs=[first] + [VMEM] * (len(args) - 1),
        out_specs=out_specs or jax.tree.map(lambda _: VMEM, outs),
        scratch_shapes=list(scratch),
        cost_estimate=pl.CostEstimate(flops=1_000_000, bytes_accessed=1 << 18, transcendentals=0),
        input_output_aliases=aliases or {},
        compiler_params=pltpu.CompilerParams(vmem_limit_bytes=vmem << 20),
    )(*args)


def pairwise(value, distance, late):
    count = lax.axis_size("vox")
    pairs = [(i, ((i + late) ^ distance) - late) for i in range(count)]
    return lax.ppermute(value, "vox", [(i, j) for i, j in pairs if 0 <= j < count])


def on_device(series, live_mask, neighbours, start_vectors):
    subjects, width, frames = series.shape
    offsets = neighbours.shape[1]
    vecs = start_vectors.shape[1]
    shape = jax.ShapeDtypeStruct
    f32 = jnp.float32
    groups = lax.axis_size("subj")
    scale = 0.5 / math.sqrt(frames * subjects * groups)
    rows = -(-(offsets + 1) // 8) * 8
    smem = pl.BlockSpec(memory_space=pltpu.SMEM)
    number = lax.axis_index("vox").astype(jnp.int32)
    flags = jnp.stack([number % UNIT, (number // UNIT) % 2])
    square = pltpu.VMEM((width, width), f32)

    arriving = shifted(series, "vox", 1)

    data, marks = call(
        own_data_kernel,
        (shape((vecs + rows, width), f32), shape((offsets, width), jnp.int32)),
        start_vectors.T,
        neighbours.T,
        live_mask[None, :],
    )
    data_partner = exchanged(data, "vox", 2)
    data_row = call(
        functools.partial(compact_kernel, vecs),
        shape((2, vecs + 2 * rows, width), jnp.bfloat16),
        data,
        data_partner,
    )
    data_rows = [pairwise(data_row, UNIT, late) for late in (0, UNIT)]
    data_same = call(
        functools.partial(stack_kernel, vecs),
        shape((6, vecs + rows, width), f32),
        flags,
        data,
        data_partner,
        *data_rows,
        first=smem,
    )
    data_other = exchanged(data_same, "vox", 1)
    blocks = 3 * UNIT
    entries = shape((blocks, width, width), jnp.int32)
    marks_scratch = pltpu.VMEM((6, rows, width), jnp.int32)
    half_which = call(
        functools.partial(same_window_kernel, offsets, vecs),
        entries,
        flags,
        data_same,
        first=smem,
        scratch=[marks_scratch],
    )
    window = call(
        functools.partial(other_window_kernel, offsets, vecs),
        (entries, shape((blocks, vecs, width), f32), shape((blocks, rows, width), f32)),
        flags,
        data_same,
        data_other,
        half_which,
        first=smem,
        scratch=[marks_scratch],
        aliases={3: 0},
    )
    z, own = call(
        functools.partial(own_kernel, offsets),
        (shape(series.shape, jnp.bfloat16), shape((rows, width), f32)),
        series,
        marks,
        scratch=[square],
    )
    partial_sums = call(
        functools.partial(earlier_kernel, offsets),
        shape((rows, width), f32),
        arriving,
        z,
        marks,
        own,
        scratch=[pltpu.VMEM(series.shape, jnp.bfloat16), square],
    )

    summed = summed_over(partial_sums, "subj")
    listed = lax.broadcasted_iota(jnp.int32, summed.shape, 0) < offsets
    present = jnp.logical_and(listed, data[vecs:, :] > 0.5)
    weight = jnp.where(present, jnp.exp(scale * summed), 0.0).astype(jnp.bfloat16)
    near = [weight]
    for r in range(1, UNIT):
        near.append(exchanged(weight, "vox", r))
    row = jnp.stack(near)
    rows_around = [pairwise(row, UNIT, late) for late in (0, UNIT)]

    y, gram = call(
        functools.partial(graph_kernel, offsets),
        (shape((vecs, width), f32), shape((vecs // 2, 2 * vecs), f32)),
        flags,
        row,
        *rows_around,
        *window,
        scratch=[
            pltpu.VMEM((blocks, 3 * width, width), jnp.bfloat16),
            pltpu.VMEM((blocks, rows, width), f32),
            pltpu.VMEM((blocks, rows, width), jnp.int32),
            pltpu.VMEM((blocks, 8, width), f32),
        ],
        first=smem,
        vmem=24,
    )
    gram = summed_over(gram, "vox", UNIT)
    inverse_factor, bound = call(
        factor_kernel,
        (shape((vecs, vecs), f32), shape((1, 1), f32)),
        gram,
        out_specs=(VMEM, smem),
        scratch=[pltpu.VMEM((vecs, 2 * vecs), f32)],
    )
    return lax.cond(
        bound[0, 0] <= WELL_CONDITIONED * vecs,
        lambda: call(solve_kernel, shape((vecs, width), f32), inverse_factor, y).T,
        lambda: step_by_step(
            summed[:offsets].T, scale, live_mask, neighbours, start_vectors
        ),
    )


def solution(mesh):
    placed = (P("subj", "vox", None), P("vox"), P("vox", None), P("vox", None))
    return jax.shard_map(
        on_device, mesh=mesh, in_specs=placed, out_specs=P("vox", None), check_vma=False
    )
```
